128 devices in a mesh: row: 8 (over y_hi, z), col: 16 (over x, y_lo, core).
Axes of the slice: x: 4, y: 4 (y_hi: 2, y_lo: 2; y = y_hi * 2 + y_lo), z: 4, core: 2. Of those that a mesh axis runs over, the one named last changes fastest.
Arguments:
- obj: float32 [2, 3072, 6144], P(None, 'row', 'col'), may hold values from -6 to 6
- probe: float32 [4, 2, 128, 128], replicated, may hold values from -3 to 3
- positions: int32 [8, 16, 8, 2], P('row', 'col'), may hold values from 0 to 383
- counts: int32 [8, 16], P('row', 'col'), may hold values from 2 to 8, as said below
- offsets: int32 [8, 4], replicated, may hold values from 0 to 3, each once within a row
- measured: float32 [8, 16, 8, 128, 128], P('row', 'col'), may hold values from 0.3 to 5
Outputs:
- new_object: float32 [2, 3072, 6144], P(None, 'row', 'col')
The draws below stay inside these ranges and needn't reach their ends.
Inputs may be any that keep to these rules, and one draw needn't show every extreme that they name: `counts`: some device uses all 8 slots. At each scan slot the beams have different offsets.
All inputs are finite; a program needn't handle non-finite values.
Results may differ from the reference program's by a relative error of at most 0.0003.
Values sent between devices are 32-bit elements; how exact they have to be, the bound alone decides.
A program may use at most 128 MiB of HBM per device.

```python
import math
import jax
import jax.numpy as jnp
from jax import lax

P_SIZE = 128
BEAMS = 4
TILE = 384
SCANS = 8
NR = 3072
NC = 6144
N_ROW = 8
N_COL = 16


def draw_counts(key, part):
    first_key, second_key = jax.random.split(key)
    drawn_counts = jax.random.randint(first_key, (N_ROW * N_COL,), max(1, SCANS // 4), SCANS + 1)
    chosen = jax.random.randint(second_key, (), 0, N_ROW * N_COL)
    filled = jnp.where(jnp.arange(N_ROW * N_COL) == chosen, SCANS, drawn_counts)
    return filled.reshape(N_ROW, N_COL).astype(jnp.int32)


def place_ends(drawn, key, least, high):
    longest = drawn.shape.index(max(drawn.shape))
    spots = []
    for shift in (0, 1):
        where = [jax.random.randint(jax.random.fold_in(key, axis), (), 0, length) for axis, length in enumerate(drawn.shape)]
        where[longest] = (where[longest] + shift) % drawn.shape[longest]
        spots.append(tuple(where))
    return drawn.at[spots[0]].set(least).at[spots[1]].set(high)


def levels(own_key, dims, shards, low, largest):
    factor_of = 1.0
    for dim, blocks in shards:
        steps = jax.random.uniform(jax.random.fold_in(jax.random.fold_in(own_key, 6), dim), (blocks,), jnp.float32, low / len(shards), largest / len(shards))
        factor_of = factor_of * jnp.repeat(jnp.exp(steps), dims[dim] // blocks).reshape((-1,) + (1,) * (len(dims) - 1 - dim))
    return factor_of


def centred(own_key, shape, scale, limit, cuts=(), held_as=jnp.bfloat16):
    array = scale * jax.random.normal(own_key, shape, jnp.float32)
    if cuts:
        array = array * levels(own_key, shape, cuts, -0.22, 0.18)
    return jnp.clip(array, -limit, limit).astype(held_as)


def setup_inputs(seed: int = 0) -> dict:
    key_list = jax.random.split(jax.random.key(seed), 7)
    obj = centred(key_list[0], (2, NR, NC), 1.0, 6.0, ((1, 8), (2, 16)), jnp.float32)
    probe = centred(key_list[1], (BEAMS, 2, P_SIZE, P_SIZE), 0.5, 3.0, (), jnp.float32)
    positions = place_ends(jax.random.randint(key_list[2], (N_ROW, N_COL, SCANS, 2), 0, TILE), jax.random.fold_in(key_list[2], 1), 0, TILE - 1).astype(jnp.int32)
    counts = draw_counts(jax.random.fold_in(key_list[6], 71), 0)
    offsets = jax.vmap(lambda own: jax.random.permutation(own, BEAMS))(jax.random.split(key_list[4], SCANS)).reshape((SCANS, BEAMS)).astype(jnp.int32)
    measured = jnp.clip(jnp.exp(math.log(5.0) - 2.8134107 * jax.random.uniform(key_list[5], (N_ROW, N_COL, SCANS, P_SIZE, P_SIZE), jnp.float32) ** levels(key_list[5], (N_ROW, N_COL, SCANS, P_SIZE, P_SIZE), ((0, 8), (1, 16)), -0.2, 0.2)), 0.3, 5.0)
    return {"obj": obj, "probe": probe, "positions": positions, "counts": counts, "offsets": offsets, "measured": measured}


EPSILON = 0.5
DAMPING = 0.5

def reference(obj, probe, positions, counts, offsets, measured):
    half = P_SIZE // 2
    padded = jnp.pad(obj, ((0, 0), (half, half), (half, half)))
    probe_c = probe[:, 0] + 1j * probe[:, 1]
    accum = jnp.zeros((3, NR + P_SIZE, NC + P_SIZE), obj.dtype)

    def device_step(accum, device):
        row_idx = (device // N_COL).astype(jnp.int32)
        col_idx = (device % N_COL).astype(jnp.int32)
        spots = positions[row_idx, col_idx]
        live = (jnp.arange(SCANS) < counts[row_idx, col_idx]).astype(obj.dtype)
        tile_rows = ((row_idx + offsets) % N_ROW * TILE).astype(jnp.int32)
        start_rows = (tile_rows + spots[:, 0][:, None]).astype(jnp.int32)
        start_cols = (col_idx * TILE + spots[:, 1][:, None] + jnp.zeros_like(start_rows)).astype(jnp.int32)
        zero_index = jnp.zeros((), jnp.int32)

        def cut(row_at, col_at):
            return lax.dynamic_slice(padded, (zero_index, row_at, col_at), (2, P_SIZE, P_SIZE))
        patches = jax.vmap(jax.vmap(cut))(start_rows, start_cols)
        patch_c = patches[:, :, 0] + 1j * patches[:, :, 1]
        exit_wave = probe_c[None] * patch_c
        far_wave = jnp.fft.fft2(exit_wave, norm='ortho')
        intensity = lax.optimization_barrier(jnp.sum(jnp.abs(far_wave) ** 2, axis=1))
        factor = measured[row_idx, col_idx] / jnp.sqrt(intensity + EPSILON)
        change = (jnp.fft.ifft2(far_wave * factor[:, None], norm='ortho') - exit_wave) * live[:, None, None, None]
        gradient = jnp.conj(probe_c)[None] * change
        illum = (jnp.abs(probe_c) ** 2)[None] * live[:, None, None, None]
        contrib = jnp.stack([jnp.real(gradient), jnp.imag(gradient), illum + jnp.zeros_like(jnp.real(gradient))], axis=2)

        def add_one(index, accum):
            slot = index // BEAMS
            beam = index % BEAMS
            start = (zero_index, start_rows[slot, beam], start_cols[slot, beam])
            current = lax.dynamic_slice(accum, start, (3, P_SIZE, P_SIZE))
            return lax.dynamic_update_slice(accum, current + contrib[slot, beam].astype(accum.dtype), start)
        accum = lax.fori_loop(0, SCANS * BEAMS, add_one, accum)
        return (accum, None)
    accum, unused = lax.scan(device_step, accum, jnp.arange(N_ROW * N_COL, dtype=jnp.int32))
    inner = accum[:, half:half + NR, half:half + NC]
    return obj + inner[:2] / (inner[2] + DAMPING)
```

```python
import functools
import math

import jax
import jax.numpy as jnp
import numpy as np
from jax import lax
from jax.experimental import pallas as pl
from jax.experimental.pallas import tpu as pltpu
from jax.sharding import PartitionSpec as P

SIDE = 128
HALF = 64
BEAMS = 4
SCANS = 8
TILE = 384
TALL = TILE + 2 * HALF
COLUMNS = TILE // SIDE
SLABS = COLUMNS + 2
EPSILON = 0.5
DAMPING = 0.5
MESH = pl.DeviceIdType.MESH
VMEM = pl.BlockSpec(memory_space=pltpu.VMEM)
SMEM = pl.BlockSpec(memory_space=pltpu.SMEM)


def tables():
    index = np.arange(SIDE)
    angle = (index[:, None] * index[None, :] % SIDE) * (2.0 * math.pi / SIDE)
    c = np.cos(angle) / math.sqrt(SIDE)
    s = np.sin(angle) / math.sqrt(SIDE)
    lane = np.block([[c, -s], [s, c]])
    both = np.stack([lane, lane.T]).astype(np.float32)
    high = both.astype(jnp.bfloat16)
    low = (both - high.astype(np.float32)).astype(jnp.bfloat16)
    return high, low


def greet(partners):
    barrier = pltpu.get_barrier_semaphore()
    for partner in partners:
        pl.semaphore_signal(barrier, inc=1, device_id=partner, device_id_type=MESH)
    pl.semaphore_wait(barrier, len(partners))


def split(x):
    high = x.astype(jnp.bfloat16)
    return high, (x - high.astype(jnp.float32)).astype(jnp.bfloat16)


def dot(a, b):
    return jnp.dot(a, b, preferred_element_type=jnp.float32)


def on_lanes(x, high, low):
    x_high, x_low = split(x)
    return dot(x_high, high) + (dot(x_low, high) + dot(x_high, low))


def on_rows(high, low, x):
    x_high, x_low = split(x)
    return dot(high, x_high) + (dot(high, x_low) + dot(low, x_high))


def lane_start(x):
    at = x + HALF
    slab = lax.div(at, SIDE)
    return slab, at - slab * SIDE


def neighbours(i, j, nr, nc):
    up, down = lax.rem(i + nr - 1, nr), lax.rem(i + 1, nr)
    left, right = lax.rem(j + nc - 1, nc), lax.rem(j + 1, nc)
    return up, down, left, right


def frame_kernel(nr, nc, obj, meta, frame, metas, pack, send, recv):
    i, j = lax.axis_index("row"), lax.axis_index("col")
    up, down, left, right = neighbours(i, j, nr, nc)
    later = [lax.rem(i + k, nr) for k in (1, 2, 3)]
    earlier = [lax.rem(i + nr - k, nr) for k in (1, 2, 3)]
    lane = lax.broadcasted_iota(jnp.int32, (TILE, SIDE), 1)
    last = TILE - SIDE
    pack[0] = jnp.where(lane < HALF, obj[0, :, 0:SIDE], pltpu.roll(obj[1, :, 0:SIDE], HALF, 1))
    pack[1] = jnp.where(lane < HALF, pltpu.roll(obj[1, :, last:TILE], HALF, 1), obj[0, :, last:TILE])
    metas[0] = meta[...]
    greet(
        [{"row": r} for r in later + earlier]
        + [{"col": left}, {"col": right}]
        + [{"row": r, "col": c} for r in (up, down) for c in (left, right)]
    )
    top, low_edge, end = TILE - HALF, HALF + TILE, SLABS - 1
    plan = [
        (pack.at[0], frame.at[0, end, HALF:low_edge], {"col": left}),
        (pack.at[1], frame.at[0, 0, HALF:low_edge], {"col": right}),
        (pack.at[0, 0:HALF], frame.at[0, end, low_edge:TALL], {"row": up, "col": left}),
        (pack.at[0, top:TILE], frame.at[0, end, 0:HALF], {"row": down, "col": left}),
        (pack.at[1, 0:HALF], frame.at[0, 0, low_edge:TALL], {"row": up, "col": right}),
        (pack.at[1, top:TILE], frame.at[0, 0, 0:HALF], {"row": down, "col": right}),
    ] + [(meta, metas.at[k + 1], {"row": later[k]}) for k in range(3)]
    for b in range(COLUMNS):
        part = slice(b * SIDE, (b + 1) * SIDE)
        plan.append((obj.at[:, 0:HALF, part], frame.at[:, b + 1, low_edge:TALL], {"row": up}))
        plan.append((obj.at[:, top:TILE, part], frame.at[:, b + 1, 0:HALF], {"row": down}))
    copies = [
        pltpu.make_async_remote_copy(
            src_ref=src, dst_ref=dst, send_sem=send.at[q], recv_sem=recv.at[q], device_id=to, device_id_type=MESH
        )
        for q, (src, dst, to) in enumerate(plan)
    ]
    for copy in copies:
        copy.start()
    for b in range(COLUMNS):
        frame[:, b + 1, HALF:low_edge] = obj[:, :, b * SIDE : (b + 1) * SIDE]
    for copy in copies:
        copy.wait()
    for slab in (0, end):
        frame[1, slab] = pltpu.roll(frame[0, slab], HALF, 1)

    @pl.when(i == 0)
    def _():
        frame[:, :, 0:HALF] = jnp.zeros((2, SLABS, HALF, SIDE), jnp.float32)

    @pl.when(i == nr - 1)
    def _():
        frame[:, :, low_edge:TALL] = jnp.zeros((2, SLABS, HALF, SIDE), jnp.float32)

    @pl.when(j == 0)
    def _():
        frame[:, 0] = jnp.zeros((2, TALL, SIDE), jnp.float32)

    @pl.when(j == nc - 1)
    def _():
        frame[:, end] = jnp.zeros((2, TALL, SIDE), jnp.float32)


def wave_kernel(nr, frame, probe, metas, offsets, measured, high, low, grads, psi, far, inten, relay, gathered, facs, send, recv):
    me = lax.axis_index("row")

    def to(by):
        return {"row": lax.rem(me + by + nr, nr)}

    greet([to(1), to(-1), to(3), to(-3)])

    def beam_at(s, k):
        beam = jnp.int32(0)
        for q in range(1, BEAMS):
            beam = jnp.where(offsets[s, q] == k, q, beam)
        return beam

    def copy(s, kind):
        odd = lax.rem(s, 2)
        near = 1 + 2 * odd
        straight = 3 - 2 * odd
        if kind == 0:
            src, dst, dev = inten.at[s, 2], relay.at[s], to(2 * odd - 1)
        elif kind == 1:
            src, dst, dev = inten.at[s, straight], gathered.at[s, 0], to(-straight)
        elif kind == 2:
            src, dst, dev = inten.at[s, near], gathered.at[s, 1], to(-near)
        elif kind == 3:
            src, dst, dev = facs.at[s, 0], facs.at[s, near], to(near)
        elif kind == 4:
            src, dst, dev = facs.at[s, 0], facs.at[s, straight], to(straight)
        else:
            src, dst, dev = facs.at[s, near], facs.at[s, 2], to(1 - 2 * odd)
        return pltpu.make_async_remote_copy(
            src_ref=src,
            dst_ref=dst,
            send_sem=send.at[s, kind],
            recv_sem=recv.at[s, kind],
            device_id=dev,
            device_id_type=MESH,
        )

    column = lax.broadcasted_iota(jnp.int32, (SIDE, SIDE), 1)

    def forward(s):
        rows = []
        for k in range(BEAMS):
            y = metas[k, s, 0]
            slab, lane = lane_start(metas[k, s, 1])
            turn = lax.rem(SIDE - lane, SIDE)
            beam = beam_at(s, k)
            z_re, z_im = [
                jnp.where(
                    column < SIDE - lane,
                    pltpu.roll(frame[c, slab, pl.ds(y, SIDE)], turn, 1),
                    pltpu.roll(frame[c, slab + 1, pl.ds(y, SIDE)], turn, 1),
                )
                for c in range(2)
            ]
            p_re, p_im = probe[beam, 0], probe[beam, 1]
            wave = jnp.concatenate([p_re * z_re - p_im * z_im, p_re * z_im + p_im * z_re], axis=1)
            psi[s, k * SIDE : (k + 1) * SIDE] = wave
            rows.append(wave)
        once = on_lanes(jnp.concatenate(rows, axis=0), high[0], low[0])
        once = jnp.concatenate(
            [
                jnp.concatenate([once[k * SIDE : (k + 1) * SIDE, q * SIDE : (q + 1) * SIDE] for k in range(BEAMS)], axis=1)
                for q in range(2)
            ],
            axis=0,
        )
        twice = on_rows(high[1], low[1], once)
        far[s] = twice
        for k in range(BEAMS):
            re = twice[:SIDE, k * SIDE : (k + 1) * SIDE]
            im = twice[SIDE:, k * SIDE : (k + 1) * SIDE]
            inten[s, k] = re * re + im * im
        copy(s, 0).start()
        copy(s, 1).start()

    def join(s):
        copy(s, 0).wait_recv()
        near = 1 + 2 * lax.rem(s, 2)
        inten[s, near] = inten[s, near] + relay[s]
        copy(s, 2).start()

    def settle(s):
        copy(s, 1).wait_recv()
        copy(s, 2).wait_recv()
        total = inten[s, 0] + gathered[s, 0] + gathered[s, 1]
        facs[s, 0] = measured[s] / jnp.sqrt(total + EPSILON)
        copy(s, 3).start()
        copy(s, 4).start()

    def hand_on(s):
        copy(s, 3).wait_recv()
        copy(s, 5).start()

    def back(s):
        copy(s, 4).wait_recv()
        copy(s, 5).wait_recv()
        factor = jnp.concatenate([facs[s, k] for k in range(BEAMS)], axis=1)
        scaled = jnp.concatenate([far[s, :SIDE] * factor, far[s, SIDE:] * factor], axis=0)
        once = on_rows(high[0], low[0], scaled)
        once = jnp.concatenate(
            [
                jnp.concatenate([once[q * SIDE : (q + 1) * SIDE, k * SIDE : (k + 1) * SIDE] for q in range(2)], axis=1)
                for k in range(BEAMS)
            ],
            axis=0,
        )
        change = on_lanes(once, high[1], low[1]) - psi[s]
        for k in range(BEAMS):
            beam = beam_at(s, k)
            p_re, p_im = probe[beam, 0], probe[beam, 1]
            c_re = change[k * SIDE : (k + 1) * SIDE, :SIDE]
            c_im = change[k * SIDE : (k + 1) * SIDE, SIDE:]
            grads[s, k * SIDE : (k + 1) * SIDE, :SIDE] = p_re * c_re + p_im * c_im
            grads[s, k * SIDE : (k + 1) * SIDE, SIDE:] = p_re * c_im - p_im * c_re

    stages = ((forward, 0), (join, 1), (settle, 2), (hand_on, 3), (back, 4))

    def step(t, carry):
        for stage, lag in stages:

            @pl.when(jnp.logical_and(t >= lag, t < SCANS + lag))
            def _(stage=stage, lag=lag):
                stage(t - lag)

        return carry

    lax.fori_loop(0, SCANS + stages[-1][1], step, 0)

    def drain(s, carry):
        for kind in range(6):
            copy(s, kind).wait_send()
        return carry

    lax.fori_loop(0, SCANS, drain, 0)


def place_kernel(grads, probe, metas, offsets, accum, illum):
    for b in range(BEAMS):
        illum[b] = probe[b, 0] * probe[b, 0] + probe[b, 1] * probe[b, 1]
    accum[...] = jnp.zeros_like(accum)
    column = lax.broadcasted_iota(jnp.int32, (SIDE, SIDE), 1)

    def add_one(q, carry):
        s, k = lax.div(q, BEAMS), lax.rem(q, BEAMS)

        @pl.when(s < metas[k, 0, 2])
        def _():
            y = metas[k, s, 0]
            slab, lane = lane_start(metas[k, s, 1])
            beam = jnp.int32(0)
            for b in range(1, BEAMS):
                beam = jnp.where(offsets[s, b] == k, b, beam)
            at = pl.ds(pl.multiple_of(k * SIDE, SIDE), SIDE)
            parts = (grads[s, at, :SIDE], grads[s, at, SIDE:], illum[beam])
            for channel, part in enumerate(parts):
                turned = pltpu.roll(part, lane, 1)
                here, there = (channel, slab, pl.ds(y, SIDE)), (channel, slab + 1, pl.ds(y, SIDE))
                accum[here] = accum[here] + jnp.where(column >= lane, turned, 0.0)
                accum[there] = accum[there] + jnp.where(column < lane, turned, 0.0)

        return carry

    lax.fori_loop(0, SCANS * BEAMS, add_one, 0)


def rim_kernel(nr, nc, accum, obj, out, pack, rows_in, sides_in, weights_in, send, recv):
    i, j = lax.axis_index("row"), lax.axis_index("col")
    up, down, left, right = neighbours(i, j, nr, nc)
    low_edge, top, end = HALF + TILE, TILE - HALF, SLABS - 1
    lane = lax.broadcasted_iota(jnp.int32, (TALL, SIDE), 1)
    pack[0] = jnp.where(lane >= HALF, accum[0, 0], pltpu.roll(accum[1, 0], HALF, 1))
    pack[1] = jnp.where(lane < HALF, accum[0, end], pltpu.roll(accum[1, end], HALF, 1))
    greet(
        [{"row": up}, {"row": down}, {"col": left}, {"col": right}]
        + [{"row": r, "col": c} for r in (up, down) for c in (left, right)]
    )
    plan = [
        (accum.at[:, 1:end, 0:HALF], rows_in.at[1], {"row": up}),
        (accum.at[:, 1:end, low_edge:TALL], rows_in.at[0], {"row": down}),
    ]
    ends = ((0, HALF, low_edge, up), (HALF, low_edge, HALF, None), (low_edge, TALL, 0, down))
    for side, (slab, to_col) in enumerate(((0, left), (end, right))):
        for first, stop, land, to_row in ends:
            to = {"col": to_col} if to_row is None else {"row": to_row, "col": to_col}
            arrive = slice(land, land + stop - first)
            plan.append((pack.at[side, first:stop], sides_in.at[side, arrive], to))
            plan.append((accum.at[2, slab, first:stop], weights_in.at[side, arrive], to))
    copies = [
        pltpu.make_async_remote_copy(
            src_ref=src, dst_ref=dst, send_sem=send.at[q], recv_sem=recv.at[q], device_id=to, device_id_type=MESH
        )
        for q, (src, dst, to) in enumerate(plan)
    ]
    for copy in copies:
        copy.start()
    for copy in copies:
        copy.wait()

    def kept(ok, value):
        return jnp.where(ok, value, 0.0)

    lane = lax.broadcasted_iota(jnp.int32, (TILE, SIDE), 1)

    def gather(head, middle, tail):
        return jnp.concatenate([head, middle, tail], axis=0)

    def column(ref, side):
        head = ref[side, HALF:SIDE] + kept(i > 0, ref[side, 0:HALF])
        tail = ref[side, TILE:low_edge] + kept(i < nr - 1, ref[side, low_edge:TALL])
        return gather(head, ref[side, SIDE:TILE], tail)

    from_right, from_left = column(sides_in, 0), column(sides_in, 1)
    rights = (from_right, pltpu.roll(from_right, HALF, 1), column(weights_in, 0))
    lefts = (from_left, pltpu.roll(from_left, HALF, 1), column(weights_in, 1))
    for b in range(COLUMNS):
        sums = []
        for c in range(3):
            head = accum[c, b + 1, HALF:SIDE] + kept(i > 0, rows_in[0, c, b])
            tail = accum[c, b + 1, TILE:low_edge] + kept(i < nr - 1, rows_in[1, c, b])
            value = gather(head, accum[c, b + 1, SIDE:TILE], tail)
            if b == 0:
                value = value + kept(jnp.logical_and(lane < HALF, j > 0), lefts[c])
            if b == COLUMNS - 1:
                value = value + kept(jnp.logical_and(lane >= HALF, j < nc - 1), rights[c])
            sums.append(value)
        part = slice(b * SIDE, (b + 1) * SIDE)
        for c in range(2):
            out[c, :, part] = obj[c, :, part] + sums[c] / (sums[2] + DAMPING)


def params(collective_id, mebibytes):
    return pltpu.CompilerParams(
        collective_id=collective_id, has_side_effects=True, vmem_limit_bytes=mebibytes * 2**20
    )


def f32(*shape):
    return jax.ShapeDtypeStruct(shape, jnp.float32)


def on_device(obj, probe, positions, counts, offsets, measured):
    nr, nc = lax.axis_size("row"), lax.axis_size("col")
    spots = positions[0, 0]
    count = jnp.broadcast_to(counts, (SCANS, 1))
    meta = jnp.pad(jnp.concatenate([spots, count], axis=1), ((0, 0), (0, SIDE - 3)))
    dma = pltpu.SemaphoreType.DMA
    frame, metas = pl.pallas_call(
        functools.partial(frame_kernel, nr, nc),
        out_shape=(f32(2, SLABS, TALL, SIDE), jax.ShapeDtypeStruct((BEAMS, SCANS, SIDE), jnp.int32)),
        in_specs=[VMEM, VMEM],
        out_specs=(VMEM, VMEM),
        scratch_shapes=[pltpu.VMEM((2, TILE, SIDE), jnp.float32), dma((15,)), dma((15,))],
        compiler_params=params(1, 16),
        name="frame",
    )(obj, meta)
    high, low = tables()
    block = (SIDE, SIDE)
    grads = pl.pallas_call(
        functools.partial(wave_kernel, nr),
        out_shape=f32(SCANS, BEAMS * SIDE, 2 * SIDE),
        in_specs=[VMEM, VMEM, SMEM, SMEM, VMEM, VMEM, VMEM],
        out_specs=VMEM,
        scratch_shapes=[
            pltpu.VMEM((SCANS, BEAMS * SIDE, 2 * SIDE), jnp.float32),
            pltpu.VMEM((SCANS, 2 * SIDE, BEAMS * SIDE), jnp.float32),
            pltpu.VMEM((SCANS, BEAMS) + block, jnp.float32),
            pltpu.VMEM((SCANS,) + block, jnp.float32),
            pltpu.VMEM((SCANS, 2) + block, jnp.float32),
            pltpu.VMEM((SCANS, BEAMS) + block, jnp.float32),
            dma((SCANS, 6)),
            dma((SCANS, 6)),
        ],
        compiler_params=params(2, 40),
        name="wave",
    )(frame, probe, metas, offsets, measured[0, 0], jnp.asarray(high), jnp.asarray(low))
    accum = pl.pallas_call(
        place_kernel,
        out_shape=f32(3, SLABS, TALL, SIDE),
        in_specs=[VMEM, VMEM, SMEM, SMEM],
        out_specs=VMEM,
        scratch_shapes=[pltpu.VMEM((BEAMS,) + block, jnp.float32)],
        compiler_params=pltpu.CompilerParams(vmem_limit_bytes=24 * 2**20),
        name="place",
    )(grads, probe, metas, offsets)
    return pl.pallas_call(
        functools.partial(rim_kernel, nr, nc),
        out_shape=f32(2, TILE, TILE),
        in_specs=[VMEM, VMEM],
        out_specs=VMEM,
        scratch_shapes=[
            pltpu.VMEM((2, TALL, SIDE), jnp.float32),
            pltpu.VMEM((2, 3, COLUMNS, HALF, SIDE), jnp.float32),
            pltpu.VMEM((2, TALL, SIDE), jnp.float32),
            pltpu.VMEM((2, TALL, SIDE), jnp.float32),
            dma((14,)),
            dma((14,)),
        ],
        compiler_params=params(3, 24),
        name="rim",
    )(accum, obj)


def solution(mesh):
    return jax.shard_map(
        on_device,
        mesh=mesh,
        in_specs=(
            P(None, "row", "col"),
            P(),
            P("row", "col", None, None),
            P("row", "col"),
            P(),
            P("row", "col", None, None, None),
        ),
        out_specs=P(None, "row", "col"),
        check_vma=False,
    )
```

```python
import functools
import math

import jax
import jax.numpy as jnp
import numpy as np
from jax import lax
from jax.experimental import pallas as pl
from jax.experimental.pallas import tpu as pltpu
from jax.sharding import PartitionSpec as P

SIDE = 128
HALF = 64
BEAMS = 4
SCANS = 8
TILE = 384
TALL = TILE + 2 * HALF
COLUMNS = TILE // SIDE
SLABS = COLUMNS + 2
EPSILON = 0.5
DAMPING = 0.5
MESH = pl.DeviceIdType.MESH
VMEM = pl.BlockSpec(memory_space=pltpu.VMEM)
SMEM = pl.BlockSpec(memory_space=pltpu.SMEM)
ANY = pl.BlockSpec(memory_space=pl.ANY)
PAD = 512
STAGES = (("forward", 0), ("weigh", 2), ("join", 2), ("settle", 4), ("hand_on", 6), ("back", 8))
WEIGHTS_AT = 12


def tables():
    index = np.arange(SIDE)
    angle = (index[:, None] * index[None, :] % SIDE) * (2.0 * math.pi / SIDE)
    c = np.cos(angle) / math.sqrt(SIDE)
    s = np.sin(angle) / math.sqrt(SIDE)
    lane = np.block([[c, -s], [s, c]])
    both = np.stack([lane, lane.T]).astype(np.float32)
    high = both.astype(jnp.bfloat16)
    low = (both - high.astype(np.float32)).astype(jnp.bfloat16)
    return high, low


def split(x):
    high = x.astype(jnp.bfloat16)
    return high, (x - high.astype(jnp.float32)).astype(jnp.bfloat16)


def dot(a, b):
    return jnp.dot(a, b, preferred_element_type=jnp.float32)


def on_lanes(x, high, low):
    x_high, x_low = split(x)
    return dot(x_high, high) + (dot(x_low, high) + dot(x_high, low))


def on_rows(high, low, x):
    x_high, x_low = split(x)
    return dot(high, x_high) + (dot(high, x_low) + dot(low, x_high))


def lane_start(x):
    at = x + HALF
    slab = lax.div(at, SIDE)
    return slab, at - slab * SIDE


def ROUTE(z, s):
    return lax.rem(s, 2)


def neighbours(i, j, nr, nc):
    up, down = lax.rem(i + nr - 1, nr), lax.rem(i + 1, nr)
    left, right = lax.rem(j + nc - 1, nc), lax.rem(j + 1, nc)
    return up, down, left, right


def step_kernel(
    nr, nc, obj_hbm, probe_hbm, measured_hbm, high_hbm, low_hbm, meta, offsets, out,
    obj, probe, measured, high, low, metas_in, metas, frame, pack, psi, far, inten, relay, gathered, facs,
    padded, accum, rows_in, sides_in, weight_rows, weight_sides, local, send, recv, wave_send, wave_recv,
):
    i, j = lax.axis_index("row"), lax.axis_index("col")
    up, down, left, right = neighbours(i, j, nr, nc)
    later = [lax.rem(i + k, nr) for k in (1, 2, 3)]
    earlier = [lax.rem(i + nr - k, nr) for k in (1, 2, 3)]
    corners = [{"row": r, "col": c} for r in (up, down) for c in (left, right)]
    partners = [{"row": r} for r in later + earlier] + [{"col": left}, {"col": right}] + corners
    barrier = pltpu.get_barrier_semaphore()
    for partner in partners:
        pl.semaphore_signal(barrier, inc=1, device_id=partner, device_id_type=MESH)
    fetches = [
        pltpu.make_async_copy(src, dst, local.at[q])
        for q, (src, dst) in enumerate(
            ((obj_hbm, obj), (probe_hbm, probe), (high_hbm, high), (low_hbm, low), (measured_hbm, measured))
        )
    ]
    for fetch in fetches:
        fetch.start()
    metas_in[0] = meta[...]

    def clear(q, carry):
        padded[q] = jnp.zeros((2 * PAD, SIDE), jnp.float32)
        return carry

    lax.fori_loop(0, 4 * BEAMS + 1, clear, 0)

    def clear_sum(q, carry):
        accum[lax.div(q, SLABS), lax.rem(q, SLABS)] = jnp.zeros((TALL, SIDE), jnp.float32)
        return carry

    lax.fori_loop(0, 3 * SLABS, clear_sum, 0)
    fetches[0].wait()
    lane = lax.broadcasted_iota(jnp.int32, (TILE, SIDE), 1)
    low_edge, top, end, last = HALF + TILE, TILE - HALF, SLABS - 1, TILE - SIDE
    pack[0, HALF:low_edge] = jnp.where(lane < HALF, obj[0, :, 0:SIDE], pltpu.roll(obj[1, :, 0:SIDE], HALF, 1))
    pack[1, HALF:low_edge] = jnp.where(lane < HALF, pltpu.roll(obj[1, :, last:TILE], HALF, 1), obj[0, :, last:TILE])
    pl.semaphore_wait(barrier, len(partners))

    def exchange(plan, first):
        copies = [
            pltpu.make_async_remote_copy(
                src_ref=src,
                dst_ref=dst,
                send_sem=send.at[first + q],
                recv_sem=recv.at[first + q],
                device_id=dev,
                device_id_type=MESH,
            )
            for q, (src, dst, dev) in enumerate(plan)
        ]
        for one in copies:
            one.start()
        return copies

    heads, tails = slice(HALF, SIDE), slice(TILE, low_edge)
    plan = [(meta, metas_in.at[k + 1], {"row": later[k]}) for k in range(3)]
    for b in range(COLUMNS):
        part = slice(b * SIDE, (b + 1) * SIDE)
        plan.append((obj.at[:, 0:HALF, part], frame.at[:, b + 1, low_edge:TALL], {"row": up}))
        plan.append((obj.at[:, top:TILE, part], frame.at[:, b + 1, 0:HALF], {"row": down}))
    plan += [
        (pack.at[0, HALF:low_edge], frame.at[0, end, HALF:low_edge], {"col": left}),
        (pack.at[1, HALF:low_edge], frame.at[0, 0, HALF:low_edge], {"col": right}),
        (pack.at[0, heads], frame.at[0, end, low_edge:TALL], {"row": up, "col": left}),
        (pack.at[0, tails], frame.at[0, end, 0:HALF], {"row": down, "col": left}),
        (pack.at[1, heads], frame.at[0, 0, low_edge:TALL], {"row": up, "col": right}),
        (pack.at[1, tails], frame.at[0, 0, 0:HALF], {"row": down, "col": right}),
    ]
    copies = exchange(plan, 0)
    for b in range(COLUMNS):
        frame[:, b + 1, HALF:low_edge] = obj[:, :, b * SIDE : (b + 1) * SIDE]
    for fetch in fetches[1:]:
        fetch.wait()
    for one in copies[:3]:
        one.wait()
    settled = pltpu.make_async_copy(metas_in, metas, local.at[5])
    settled.start()
    for one in copies[3:]:
        one.wait()
    settled.wait()
    for slab in (0, end):
        frame[1, slab] = pltpu.roll(frame[0, slab], HALF, 1)

    @pl.when(i == 0)
    def _():
        frame[:, :, 0:HALF] = jnp.zeros((2, SLABS, HALF, SIDE), jnp.float32)

    @pl.when(i == nr - 1)
    def _():
        frame[:, :, low_edge:TALL] = jnp.zeros((2, SLABS, HALF, SIDE), jnp.float32)

    @pl.when(j == 0)
    def _():
        frame[:, 0] = jnp.zeros((2, TALL, SIDE), jnp.float32)

    @pl.when(j == nc - 1)
    def _():
        frame[:, end] = jnp.zeros((2, TALL, SIDE), jnp.float32)

    def to(by):
        return {"row": lax.rem(i + by + nr, nr)}

    def by_third(s, k):
        return ROUTE(lax.rem(i + nr - k, 4), s)

    def copy(s, kind):
        if kind == 0:
            src, dst, dev = inten.at[s, 2], relay.at[s, 0], to(-1)
        elif kind == 1:
            src, dst, dev = inten.at[s, 2], relay.at[s, 1], to(1)
        elif kind == 2:
            src, dst, dev = inten.at[s, 1], gathered.at[s, 0], to(-1)
        elif kind == 3:
            src, dst, dev = inten.at[s, 3], gathered.at[s, 1], to(-3)
        elif kind == 4:
            src, dst, dev = facs.at[s, 0], facs.at[s, 1], to(1)
        elif kind == 5:
            src, dst, dev = facs.at[s, 0], facs.at[s, 3], to(3)
        elif kind == 6:
            src, dst, dev = facs.at[s, 1], facs.at[s, 2], to(1)
        else:
            src, dst, dev = facs.at[s, 3], facs.at[s, 2], to(-1)
        place = 6 if kind == 7 else kind
        return pltpu.make_async_remote_copy(
            src_ref=src,
            dst_ref=dst,
            send_sem=wave_send.at[s, kind],
            recv_sem=wave_recv.at[s, place],
            device_id=dev,
            device_id_type=MESH,
        )

    def beam_at(s, k):
        beam = jnp.int32(0)
        for q in range(1, BEAMS):
            beam = jnp.where(offsets[s, q] == k, q, beam)
        return beam

    column = lax.broadcasted_iota(jnp.int32, (SIDE, SIDE), 1)

    def forward(s):
        rows = []
        for k in range(BEAMS):
            y = metas[k, s, 0]
            slab, shift = lane_start(metas[k, s, 1])
            turn = lax.rem(SIDE - shift, SIDE)
            beam = beam_at(s, k)
            z_re, z_im = [
                jnp.where(
                    column < SIDE - shift,
                    pltpu.roll(frame[c, slab, pl.ds(y, SIDE)], turn, 1),
                    pltpu.roll(frame[c, slab + 1, pl.ds(y, SIDE)], turn, 1),
                )
                for c in range(2)
            ]
            p_re, p_im = probe[beam, 0], probe[beam, 1]
            wave = jnp.concatenate([p_re * z_re - p_im * z_im, p_re * z_im + p_im * z_re], axis=1)
            psi[s, k * SIDE : (k + 1) * SIDE] = wave
            rows.append(wave)
        once = on_lanes(jnp.concatenate(rows, axis=0), high[0], low[0])
        once = jnp.concatenate(
            [
                jnp.concatenate([once[k * SIDE : (k + 1) * SIDE, q * SIDE : (q + 1) * SIDE] for k in range(BEAMS)], axis=1)
                for q in range(2)
            ],
            axis=0,
        )
        twice = on_rows(high[1], low[1], once)
        far[s] = twice
        for k in (2, 1, 3, 0):
            re = twice[:SIDE, k * SIDE : (k + 1) * SIDE]
            im = twice[SIDE:, k * SIDE : (k + 1) * SIDE]
            inten[s, k] = re * re + im * im
        for kind, wanted in ((0, by_third(s, 2) == 0), (1, by_third(s, 2) == 1), (2, by_third(s, 1) == 1), (3, by_third(s, 3) == 0)):

            @pl.when(wanted)
            def _(kind=kind):
                copy(s, kind).start()

    def join(s):
        for k, which, wanted in ((1, 0, by_third(s, 1) == 0), (3, 1, by_third(s, 3) == 1)):

            @pl.when(wanted)
            def _(k=k, which=which):
                copy(s, which).wait_recv()
                inten[s, k] = inten[s, k] + relay[s, which]
                copy(s, 2 + which).start()

    def settle(s):
        copy(s, 2).wait_recv()
        copy(s, 3).wait_recv()
        total = inten[s, 0] + gathered[s, 0] + gathered[s, 1]
        facs[s, 0] = measured[s] / jnp.sqrt(total + EPSILON)
        copy(s, 4).start()
        copy(s, 5).start()

    def hand_on(s):
        for k, which, wanted in ((1, 0, by_third(s, 1) == 0), (3, 1, by_third(s, 3) == 1)):

            @pl.when(wanted)
            def _(k=k, which=which):
                copy(s, 4 + which).wait_recv()
                copy(s, 6 + which).start()

    def place(s, channels):
        starts, picks = [], []
        for k in range(BEAMS):
            slab, shift = lane_start(metas[k, s, 1])
            starts.append(PAD - metas[k, s, 0])
            live = s < metas[k, 0, 2]
            for q, (channel, values) in enumerate(channels):
                turned = pltpu.roll(jnp.where(live, values[k], 0.0), shift, 1)
                at = 2 * (q * BEAMS + k)
                padded[at, PAD : PAD + SIDE] = jnp.where(column >= shift, turned, 0.0)
                padded[at + 1, PAD : PAD + SIDE] = jnp.where(column < shift, turned, 0.0)
            picks.append([jnp.where(slab == b, 0, jnp.where(slab + 1 == b, 1, 2)) for b in range(SLABS)])
        for q, (channel, values) in enumerate(channels):

            def add(row, carry, q=q, channel=channel):
                here = pl.ds(pl.multiple_of(row * HALF, HALF), HALF)
                for b in range(SLABS):
                    value = accum[channel, b, here]
                    for k in range(BEAMS):
                        at = jnp.where(picks[k][b] == 2, 4 * BEAMS, 2 * (q * BEAMS + k) + picks[k][b])
                        value = value + padded[at, pl.ds(starts[k] + row * HALF, HALF)]
                    accum[channel, b, here] = value
                return carry

            lax.fori_loop(0, TALL // HALF, add, 0)

    def weigh(s):
        values = []
        for k in range(BEAMS):
            beam = beam_at(s, k)
            p_re, p_im = probe[beam, 0], probe[beam, 1]
            values.append(p_re * p_re + p_im * p_im)
        place(s, [(2, values)])

    def back(s):
        for k, which, wanted in ((1, 0, by_third(s, 1) == 1), (3, 1, by_third(s, 3) == 0)):

            @pl.when(wanted)
            def _(which=which):
                copy(s, 4 + which).wait_recv()

        copy(s, 6).wait_recv()
        factor = jnp.concatenate([facs[s, k] for k in range(BEAMS)], axis=1)
        scaled = jnp.concatenate([far[s, :SIDE] * factor, far[s, SIDE:] * factor], axis=0)
        once = on_rows(high[0], low[0], scaled)
        once = jnp.concatenate(
            [
                jnp.concatenate([once[q * SIDE : (q + 1) * SIDE, k * SIDE : (k + 1) * SIDE] for q in range(2)], axis=1)
                for k in range(BEAMS)
            ],
            axis=0,
        )
        change = on_lanes(once, high[1], low[1]) - psi[s]
        re, im = [], []
        for k in range(BEAMS):
            beam = beam_at(s, k)
            p_re, p_im = probe[beam, 0], probe[beam, 1]
            c_re = change[k * SIDE : (k + 1) * SIDE, :SIDE]
            c_im = change[k * SIDE : (k + 1) * SIDE, SIDE:]
            re.append(p_re * c_re + p_im * c_im)
            im.append(p_re * c_im - p_im * c_re)
        place(s, [(0, re), (1, im)])

    ends = ((0, HALF, low_edge, up), (HALF, low_edge, HALF, None), (low_edge, TALL, 0, down))
    sides = ((0, left), (end, right))
    weight_plan = [
        (accum.at[2, 1:end, 0:HALF], weight_rows.at[1], {"row": up}),
        (accum.at[2, 1:end, low_edge:TALL], weight_rows.at[0], {"row": down}),
    ]
    rim_plan = [
        (accum.at[0:2, 1:end, 0:HALF], rows_in.at[1], {"row": up}),
        (accum.at[0:2, 1:end, low_edge:TALL], rows_in.at[0], {"row": down}),
    ]
    for side, (slab, to_col) in enumerate(sides):
        for first, stop, land, to_row in ends:
            dev = {"col": to_col} if to_row is None else {"row": to_row, "col": to_col}
            arrive = slice(land, land + stop - first)
            weight_plan.append((accum.at[2, slab, first:stop], weight_sides.at[side, arrive], dev))
            rim_plan.append((pack.at[side, first:stop], sides_in.at[side, arrive], dev))
    work = {"forward": forward, "weigh": weigh, "join": join, "settle": settle, "hand_on": hand_on, "back": back}

    def step(t, carry):
        for name, lag in STAGES:

            @pl.when(jnp.logical_and(t >= lag, t < SCANS + lag))
            def _(name=name, lag=lag):
                work[name](t - lag)

        @pl.when(t == WEIGHTS_AT)
        def _():
            exchange(weight_plan, 15)

        return carry

    lax.fori_loop(0, SCANS + STAGES[-1][1], step, 0)
    lane = lax.broadcasted_iota(jnp.int32, (TALL, SIDE), 1)
    pack[0] = jnp.where(lane >= HALF, accum[0, 0], pltpu.roll(accum[1, 0], HALF, 1))
    pack[1] = jnp.where(lane < HALF, accum[0, end], pltpu.roll(accum[1, end], HALF, 1))
    copies = exchange(rim_plan, 23)
    waits = [
        pltpu.make_async_remote_copy(
            src_ref=src, dst_ref=dst, send_sem=send.at[15 + q], recv_sem=recv.at[15 + q], device_id=dev, device_id_type=MESH
        )
        for q, (src, dst, dev) in enumerate(weight_plan)
    ]
    for one in waits:
        one.wait()

    def drain(s, carry):
        for kind in (2, 3, 4, 5):
            copy(s, kind).wait_send()
        for kind, wanted in (
            (0, by_third(s, 2) == 0),
            (1, by_third(s, 2) == 1),
            (6, by_third(s, 1) == 0),
            (7, by_third(s, 3) == 1),
        ):

            @pl.when(wanted)
            def _(kind=kind):
                copy(s, kind).wait_send()

        return carry

    lax.fori_loop(0, SCANS, drain, 0)
    for one in copies:
        one.wait()

    def kept(ok, value):
        return jnp.where(ok, value, 0.0)

    lane = lax.broadcasted_iota(jnp.int32, (TILE, SIDE), 1)

    def rim_column(ref, side):
        head = ref[side, HALF:SIDE] + kept(i > 0, ref[side, 0:HALF])
        tail = ref[side, TILE:low_edge] + kept(i < nr - 1, ref[side, low_edge:TALL])
        return jnp.concatenate([head, ref[side, SIDE:TILE], tail], axis=0)

    from_right, from_left = rim_column(sides_in, 0), rim_column(sides_in, 1)
    rights = (from_right, pltpu.roll(from_right, HALF, 1), rim_column(weight_sides, 0))
    lefts = (from_left, pltpu.roll(from_left, HALF, 1), rim_column(weight_sides, 1))
    for b in range(COLUMNS):
        sums = []
        for c in range(3):
            above = weight_rows[0, b] if c == 2 else rows_in[0, c, b]
            below = weight_rows[1, b] if c == 2 else rows_in[1, c, b]
            head = accum[c, b + 1, HALF:SIDE] + kept(i > 0, above)
            tail = accum[c, b + 1, TILE:low_edge] + kept(i < nr - 1, below)
            value = jnp.concatenate([head, accum[c, b + 1, SIDE:TILE], tail], axis=0)
            if b == 0:
                value = value + kept(jnp.logical_and(lane < HALF, j > 0), lefts[c])
            if b == COLUMNS - 1:
                value = value + kept(jnp.logical_and(lane >= HALF, j < nc - 1), rights[c])
            sums.append(value)
        part = slice(b * SIDE, (b + 1) * SIDE)
        for c in range(2):
            out[c, :, part] = obj[c, :, part] + sums[c] / (sums[2] + DAMPING)


def f32(*shape):
    return pltpu.VMEM(shape, jnp.float32)


def on_device(obj, probe, positions, counts, offsets, measured):
    nr, nc = lax.axis_size("row"), lax.axis_size("col")
    spots = positions[0, 0]
    count = jnp.broadcast_to(counts, (SCANS, 1))
    meta = jnp.pad(jnp.concatenate([spots, count], axis=1), ((0, 0), (0, SIDE - 3)))
    high, low = tables()
    dma = pltpu.SemaphoreType.DMA
    return pl.pallas_call(
        functools.partial(step_kernel, nr, nc),
        out_shape=jax.ShapeDtypeStruct((2, TILE, TILE), jnp.float32),
        in_specs=[ANY] * 5 + [VMEM, SMEM],
        out_specs=VMEM,
        scratch_shapes=[
            f32(2, TILE, TILE),
            f32(BEAMS, 2, SIDE, SIDE),
            f32(SCANS, SIDE, SIDE),
            pltpu.VMEM((2, 2 * SIDE, 2 * SIDE), jnp.bfloat16),
            pltpu.VMEM((2, 2 * SIDE, 2 * SIDE), jnp.bfloat16),
            pltpu.VMEM((BEAMS, SCANS, SIDE), jnp.int32),
            pltpu.SMEM((BEAMS, SCANS, SIDE), jnp.int32),
            f32(2, SLABS, TALL, SIDE),
            f32(2, TALL, SIDE),
            f32(SCANS, BEAMS * SIDE, 2 * SIDE),
            f32(SCANS, 2 * SIDE, BEAMS * SIDE),
            f32(SCANS, BEAMS, SIDE, SIDE),
            f32(SCANS, 2, SIDE, SIDE),
            f32(SCANS, 2, SIDE, SIDE),
            f32(SCANS, BEAMS, SIDE, SIDE),
            f32(4 * BEAMS + 1, 2 * PAD, SIDE),
            f32(3, SLABS, TALL, SIDE),
            f32(2, 2, COLUMNS, HALF, SIDE),
            f32(2, TALL, SIDE),
            f32(2, COLUMNS, HALF, SIDE),
            f32(2, TALL, SIDE),
            dma((6,)),
            dma((31,)),
            dma((31,)),
            dma((SCANS, 8)),
            dma((SCANS, 7)),
        ],
        compiler_params=pltpu.CompilerParams(collective_id=1, has_side_effects=True, vmem_limit_bytes=56 * 2**20),
        name="step",
    )(obj, probe, measured[0, 0], jnp.asarray(high), jnp.asarray(low), meta, offsets)


def solution(mesh):
    return jax.shard_map(
        on_device,
        mesh=mesh,
        in_specs=(
            P(None, "row", "col"),
            P(),
            P("row", "col", None, None),
            P("row", "col"),
            P(),
            P("row", "col", None, None, None),
        ),
        out_specs=P(None, "row", "col"),
        check_vma=False,
    )
```

```python
import functools
import math

import jax
import jax.numpy as jnp
import numpy as np
from jax import lax
from jax.experimental import pallas as pl
from jax.experimental.pallas import tpu as pltpu
from jax.sharding import PartitionSpec as P

SIDE = 128
HALF = 64
BEAMS = 4
SCANS = 8
TILE = 384
TALL = TILE + 2 * HALF
COLUMNS = TILE // SIDE
SLABS = COLUMNS + 2
EPSILON = 0.5
DAMPING = 0.5
MESH = pl.DeviceIdType.MESH
VMEM = pl.BlockSpec(memory_space=pltpu.VMEM)
SMEM = pl.BlockSpec(memory_space=pltpu.SMEM)
HBM = pl.BlockSpec(memory_space=pltpu.HBM)
PAD = 512
STAGES = (("forward", 0), ("join", 1), ("settle", 2), ("hand_on", 3), ("back", 4))


def tables():
    index = np.arange(SIDE)
    angle = (index[:, None] * index[None, :] % SIDE) * (2.0 * math.pi / SIDE)
    c = np.cos(angle) / math.sqrt(SIDE)
    s = np.sin(angle) / math.sqrt(SIDE)
    lane = np.block([[c, -s], [s, c]])
    both = np.stack([lane, lane.T]).astype(np.float32)
    high = both.astype(jnp.bfloat16)
    low = (both - high.astype(np.float32)).astype(jnp.bfloat16)
    return high, low


def split(x):
    high = x.astype(jnp.bfloat16)
    return high, (x - high.astype(jnp.float32)).astype(jnp.bfloat16)


def dot(a, b):
    return jnp.dot(a, b, preferred_element_type=jnp.float32)


def on_lanes(x, high, low):
    x_high, x_low = split(x)
    return dot(x_high, high) + (dot(x_low, high) + dot(x_high, low))


def on_rows(high, low, x):
    x_high, x_low = split(x)
    return dot(high, x_high) + (dot(high, x_low) + dot(low, x_high))


def lane_start(x):
    at = x + HALF
    slab = lax.div(at, SIDE)
    return slab, at - slab * SIDE


def by_fourth(z, s):
    return jnp.where(z == 1, 0, jnp.where(z == 2, 1, lax.rem(s, 2)))


def neighbours(i, j, nr, nc):
    up, down = lax.rem(i + nr - 1, nr), lax.rem(i + 1, nr)
    left, right = lax.rem(j + nc - 1, nc), lax.rem(j + 1, nc)
    return up, down, left, right


def step_kernel(
    nr, nc, obj_hbm, probe_hbm, measured_hbm, high_hbm, low_hbm, positions, counts, offsets, out,
    obj, probe, measured, high, low, meta, metas_in, metas, frame, pack, psi, far, inten, relay, gathered, facs,
    padded, accum, rows_in, sides_in, weight_pack, weight_rows, weight_sides, local, send, recv, wave_send, wave_recv,
):
    i, j = lax.axis_index("row"), lax.axis_index("col")
    up, down, left, right = neighbours(i, j, nr, nc)
    later = [lax.rem(i + k, nr) for k in (1, 2, 3)]
    earlier = [lax.rem(i + nr - k, nr) for k in (1, 2, 3)]
    corners = [{"row": r, "col": c} for r in (up, down) for c in (left, right)]
    partners = [{"row": r} for r in later + earlier] + [{"col": left}, {"col": right}] + corners
    barrier = pltpu.get_barrier_semaphore()
    for partner in partners:
        pl.semaphore_signal(barrier, inc=1, device_id=partner, device_id_type=MESH)
    fetches = [
        pltpu.make_async_copy(src, dst, local.at[q])
        for q, (src, dst) in enumerate(
            ((obj_hbm, obj), (probe_hbm, probe), (high_hbm, high), (low_hbm, low), (measured_hbm, measured))
        )
    ]
    for fetch in fetches:
        fetch.start()
    row, item = [lax.broadcasted_iota(jnp.int32, (SCANS, SIDE), d) for d in range(2)]
    packed = jnp.where(item == 2, counts[0, 0], 0)
    for s in range(SCANS):
        for c in range(2):
            packed = jnp.where(jnp.logical_and(row == s, item == c), positions[c, s], packed)
    meta[...] = packed
    metas_in[0] = packed
    fetches[0].wait()
    lane = lax.broadcasted_iota(jnp.int32, (TILE, SIDE), 1)
    low_edge, top, end, last = HALF + TILE, TILE - HALF, SLABS - 1, TILE - SIDE
    pack[0, HALF:low_edge] = jnp.where(lane < HALF, obj[0, :, 0:SIDE], pltpu.roll(obj[1, :, 0:SIDE], HALF, 1))
    pack[1, HALF:low_edge] = jnp.where(lane < HALF, pltpu.roll(obj[1, :, last:TILE], HALF, 1), obj[0, :, last:TILE])
    pl.semaphore_wait(barrier, len(partners))

    def exchange(plan, first):
        copies = [
            pltpu.make_async_remote_copy(
                src_ref=src,
                dst_ref=dst,
                send_sem=send.at[first + q],
                recv_sem=recv.at[first + q],
                device_id=dev,
                device_id_type=MESH,
            )
            for q, (src, dst, dev) in enumerate(plan)
        ]
        for one in copies:
            one.start()
        return copies

    heads, tails = slice(HALF, SIDE), slice(TILE, low_edge)
    plan = [(meta, metas_in.at[k + 1], {"row": later[k]}) for k in range(3)]
    for b in range(COLUMNS):
        part = slice(b * SIDE, (b + 1) * SIDE)
        plan.append((obj.at[:, 0:HALF, part], frame.at[:, b + 1, low_edge:TALL], {"row": up}))
        plan.append((obj.at[:, top:TILE, part], frame.at[:, b + 1, 0:HALF], {"row": down}))
    plan += [
        (pack.at[0, HALF:low_edge], frame.at[0, end, HALF:low_edge], {"col": left}),
        (pack.at[1, HALF:low_edge], frame.at[0, 0, HALF:low_edge], {"col": right}),
        (pack.at[0, heads], frame.at[0, end, low_edge:TALL], {"row": up, "col": left}),
        (pack.at[0, tails], frame.at[0, end, 0:HALF], {"row": down, "col": left}),
        (pack.at[1, heads], frame.at[0, 0, low_edge:TALL], {"row": up, "col": right}),
        (pack.at[1, tails], frame.at[0, 0, 0:HALF], {"row": down, "col": right}),
    ]
    copies = exchange(plan, 0)
    for b in range(COLUMNS):
        frame[:, b + 1, HALF:low_edge] = obj[:, :, b * SIDE : (b + 1) * SIDE]

    def clear(q, carry):
        padded[q] = jnp.zeros((2 * PAD, SIDE), jnp.float32)
        return carry

    lax.fori_loop(0, 4 * BEAMS + 1, clear, 0)

    def clear_sum(q, carry):
        accum[lax.div(q, SLABS), lax.rem(q, SLABS)] = jnp.zeros((TALL, SIDE), jnp.float32)
        return carry

    lax.fori_loop(0, 3 * SLABS, clear_sum, 0)
    for fetch in fetches[1:]:
        fetch.wait()
    for one in copies[:3]:
        one.wait()
    settled = pltpu.make_async_copy(metas_in, metas, local.at[5])
    settled.start()
    settled.wait()
    column = lax.broadcasted_iota(jnp.int32, (SIDE, SIDE), 1)

    def beam_at(s, k):
        beam = jnp.int32(0)
        for q in range(1, BEAMS):
            beam = jnp.where(offsets[q, s] == k, q, beam)
        return beam

    def place(s, channels):
        starts, picks = [], []
        for k in range(BEAMS):
            slab, shift = lane_start(metas[k, s, 1])
            starts.append(PAD - metas[k, s, 0])
            live = s < metas[k, 0, 2]
            for q, (channel, values) in enumerate(channels):
                turned = pltpu.roll(jnp.where(live, values[k], 0.0), shift, 1)
                at = 2 * (q * BEAMS + k)
                padded[at, PAD : PAD + SIDE] = jnp.where(column >= shift, turned, 0.0)
                padded[at + 1, PAD : PAD + SIDE] = jnp.where(column < shift, turned, 0.0)
            picks.append([jnp.where(slab == b, 0, jnp.where(slab + 1 == b, 1, 2)) for b in range(SLABS)])
        for q, (channel, values) in enumerate(channels):

            def add(row, carry, q=q, channel=channel):
                here = pl.ds(pl.multiple_of(row * HALF, HALF), HALF)
                for b in range(SLABS):
                    value = accum[channel, b, here]
                    for k in range(BEAMS):
                        at = jnp.where(picks[k][b] == 2, 4 * BEAMS, 2 * (q * BEAMS + k) + picks[k][b])
                        value = value + padded[at, pl.ds(starts[k] + row * HALF, HALF)]
                    accum[channel, b, here] = value
                return carry

            lax.fori_loop(0, TALL // HALF, add, 0)

    def weigh(s):
        values = []
        for k in range(BEAMS):
            beam = beam_at(s, k)
            p_re, p_im = probe[beam, 0], probe[beam, 1]
            values.append(p_re * p_re + p_im * p_im)
        place(s, [(2, values)])

    def weigh_one(s, carry):
        weigh(s)
        return carry

    lax.fori_loop(0, SCANS, weigh_one, 0)
    half_lane = lax.broadcasted_iota(jnp.int32, (HALF, SIDE), 1)
    folds = [(q * HALF, (q + 3) * HALF) for q in range(1, 4)] + [(0, low_edge)]
    for side, slab in ((0, 0), (1, end)):
        for q, (first, second) in enumerate(folds):
            straight = accum[2, slab, first : first + HALF]
            folded = pltpu.roll(accum[2, slab, second : second + HALF], HALF, 1)
            keep = half_lane >= HALF if side == 0 else half_lane < HALF
            weight_pack[side, q * HALF : (q + 1) * HALF] = jnp.where(keep, straight, folded)
    mid, fold_rows = slice(0, 3 * HALF), slice(3 * HALF, 4 * HALF)
    weight_plan = [
        (accum.at[2, 1:end, 0:HALF], weight_rows.at[1], {"row": up}),
        (accum.at[2, 1:end, low_edge:TALL], weight_rows.at[0], {"row": down}),
    ]
    for side, to_col in ((0, left), (1, right)):
        weight_plan += [
            (weight_pack.at[side, mid], weight_sides.at[side, mid], {"col": to_col}),
            (weight_pack.at[side, fold_rows], weight_sides.at[side, 4 * HALF : 5 * HALF], {"row": up, "col": to_col}),
            (weight_pack.at[side, fold_rows], weight_sides.at[side, fold_rows], {"row": down, "col": to_col}),
        ]
    weight_copies = exchange(weight_plan, 15)
    for one in copies[3:]:
        one.wait()
    for slab in (0, end):
        frame[1, slab] = pltpu.roll(frame[0, slab], HALF, 1)

    @pl.when(i == 0)
    def _():
        frame[:, :, 0:HALF] = jnp.zeros((2, SLABS, HALF, SIDE), jnp.float32)

    @pl.when(i == nr - 1)
    def _():
        frame[:, :, low_edge:TALL] = jnp.zeros((2, SLABS, HALF, SIDE), jnp.float32)

    @pl.when(j == 0)
    def _():
        frame[:, 0] = jnp.zeros((2, TALL, SIDE), jnp.float32)

    @pl.when(j == nc - 1)
    def _():
        frame[:, end] = jnp.zeros((2, TALL, SIDE), jnp.float32)

    def to(by):
        return {"row": lax.rem(i + by + nr, nr)}

    def by_third(s, k):
        return by_fourth(lax.rem(i + nr - k, 4), s)

    def copy(s, kind):
        if kind == 0:
            src, dst, dev = inten.at[s, 2], relay.at[s, 0], to(-1)
        elif kind == 1:
            src, dst, dev = inten.at[s, 2], relay.at[s, 1], to(1)
        elif kind == 2:
            src, dst, dev = inten.at[s, 1], gathered.at[s, 0], to(-1)
        elif kind == 3:
            src, dst, dev = inten.at[s, 3], gathered.at[s, 1], to(-3)
        elif kind == 4:
            src, dst, dev = facs.at[s, 0], facs.at[s, 1], to(1)
        elif kind == 5:
            src, dst, dev = facs.at[s, 0], facs.at[s, 3], to(3)
        elif kind == 6:
            src, dst, dev = facs.at[s, 1], facs.at[s, 2], to(1)
        else:
            src, dst, dev = facs.at[s, 3], facs.at[s, 2], to(-1)
        place = 6 if kind == 7 else kind
        return pltpu.make_async_remote_copy(
            src_ref=src,
            dst_ref=dst,
            send_sem=wave_send.at[s, kind],
            recv_sem=wave_recv.at[s, place],
            device_id=dev,
            device_id_type=MESH,
        )

    def forward(s):
        rows = []
        for k in range(BEAMS):
            y = metas[k, s, 0]
            slab, shift = lane_start(metas[k, s, 1])
            turn = lax.rem(SIDE - shift, SIDE)
            beam = beam_at(s, k)
            z_re, z_im = [
                jnp.where(
                    column < SIDE - shift,
                    pltpu.roll(frame[c, slab, pl.ds(y, SIDE)], turn, 1),
                    pltpu.roll(frame[c, slab + 1, pl.ds(y, SIDE)], turn, 1),
                )
                for c in range(2)
            ]
            p_re, p_im = probe[beam, 0], probe[beam, 1]
            wave = jnp.concatenate([p_re * z_re - p_im * z_im, p_re * z_im + p_im * z_re], axis=1)
            psi[s, k * SIDE : (k + 1) * SIDE] = wave
            rows.append(wave)
        once = on_lanes(jnp.concatenate(rows, axis=0), high[0], low[0])
        once = jnp.concatenate(
            [
                jnp.concatenate([once[k * SIDE : (k + 1) * SIDE, q * SIDE : (q + 1) * SIDE] for k in range(BEAMS)], axis=1)
                for q in range(2)
            ],
            axis=0,
        )
        twice = on_rows(high[1], low[1], once)
        far[s] = twice
        for k in (2, 1, 3, 0):
            re = twice[:SIDE, k * SIDE : (k + 1) * SIDE]
            im = twice[SIDE:, k * SIDE : (k + 1) * SIDE]
            inten[s, k] = re * re + im * im
        for kind, wanted in ((0, by_third(s, 2) == 0), (1, by_third(s, 2) == 1), (2, by_third(s, 1) == 1), (3, by_third(s, 3) == 0)):

            @pl.when(wanted)
            def _(kind=kind):
                copy(s, kind).start()

    def join(s):
        for k, which, wanted in ((1, 0, by_third(s, 1) == 0), (3, 1, by_third(s, 3) == 1)):

            @pl.when(wanted)
            def _(k=k, which=which):
                copy(s, which).wait_recv()
                inten[s, k] = inten[s, k] + relay[s, which]
                copy(s, 2 + which).start()

    def settle(s):
        copy(s, 2).wait_recv()
        copy(s, 3).wait_recv()
        total = inten[s, 0] + gathered[s, 0] + gathered[s, 1]
        facs[s, 0] = measured[s] / jnp.sqrt(total + EPSILON)
        copy(s, 4).start()
        copy(s, 5).start()

    def hand_on(s):
        for k, which, wanted in ((1, 0, by_third(s, 1) == 0), (3, 1, by_third(s, 3) == 1)):

            @pl.when(wanted)
            def _(k=k, which=which):
                copy(s, 4 + which).wait_recv()
                copy(s, 6 + which).start()

    def back(s):
        for k, which, wanted in ((1, 0, by_third(s, 1) == 1), (3, 1, by_third(s, 3) == 0)):

            @pl.when(wanted)
            def _(which=which):
                copy(s, 4 + which).wait_recv()

        copy(s, 6).wait_recv()
        factor = jnp.concatenate([facs[s, k] for k in range(BEAMS)], axis=1)
        scaled = jnp.concatenate([far[s, :SIDE] * factor, far[s, SIDE:] * factor], axis=0)
        once = on_rows(high[0], low[0], scaled)
        once = jnp.concatenate(
            [
                jnp.concatenate([once[q * SIDE : (q + 1) * SIDE, k * SIDE : (k + 1) * SIDE] for q in range(2)], axis=1)
                for k in range(BEAMS)
            ],
            axis=0,
        )
        change = on_lanes(once, high[1], low[1]) - psi[s]
        re, im = [], []
        for k in range(BEAMS):
            beam = beam_at(s, k)
            p_re, p_im = probe[beam, 0], probe[beam, 1]
            c_re = change[k * SIDE : (k + 1) * SIDE, :SIDE]
            c_im = change[k * SIDE : (k + 1) * SIDE, SIDE:]
            re.append(p_re * c_re + p_im * c_im)
            im.append(p_re * c_im - p_im * c_re)
        place(s, [(0, re), (1, im)])

    ends = ((0, HALF, low_edge, up), (HALF, low_edge, HALF, None), (low_edge, TALL, 0, down))
    sides = ((0, left), (end, right))
    rim_plan = [
        (accum.at[0:2, 1:end, 0:HALF], rows_in.at[1], {"row": up}),
        (accum.at[0:2, 1:end, low_edge:TALL], rows_in.at[0], {"row": down}),
    ]
    for side, (slab, to_col) in enumerate(sides):
        for first, stop, land, to_row in ends:
            dev = {"col": to_col} if to_row is None else {"row": to_row, "col": to_col}
            arrive = slice(land, land + stop - first)
            rim_plan.append((pack.at[side, first:stop], sides_in.at[side, arrive], dev))
    work = {"forward": forward, "join": join, "settle": settle, "hand_on": hand_on, "back": back}

    def step(t, carry):
        for name, lag in STAGES:

            @pl.when(jnp.logical_and(t >= lag, t < SCANS + lag))
            def _(name=name, lag=lag):
                work[name](t - lag)

        return carry

    lax.fori_loop(0, SCANS + STAGES[-1][1], step, 0)
    lane = lax.broadcasted_iota(jnp.int32, (TALL, SIDE), 1)
    pack[0] = jnp.where(lane >= HALF, accum[0, 0], pltpu.roll(accum[1, 0], HALF, 1))
    pack[1] = jnp.where(lane < HALF, accum[0, end], pltpu.roll(accum[1, end], HALF, 1))
    copies = exchange(rim_plan, 23)
    for one in weight_copies:
        one.wait()

    def drain(s, carry):
        for kind in (2, 3, 4, 5):
            copy(s, kind).wait_send()
        for kind, wanted in (
            (0, by_third(s, 2) == 0),
            (1, by_third(s, 2) == 1),
            (6, by_third(s, 1) == 0),
            (7, by_third(s, 3) == 1),
        ):

            @pl.when(wanted)
            def _(kind=kind):
                copy(s, kind).wait_send()

        return carry

    lax.fori_loop(0, SCANS, drain, 0)
    for one in copies:
        one.wait()

    def kept(ok, value):
        return jnp.where(ok, value, 0.0)

    lane = lax.broadcasted_iota(jnp.int32, (TILE, SIDE), 1)

    def rim_column(ref, side):
        head = ref[side, HALF:SIDE] + kept(i > 0, ref[side, 0:HALF])
        tail = ref[side, TILE:low_edge] + kept(i < nr - 1, ref[side, low_edge:TALL])
        return jnp.concatenate([head, ref[side, SIDE:TILE], tail], axis=0)

    from_right, from_left = rim_column(sides_in, 0), rim_column(sides_in, 1)

    def weight_column(side):
        turned = [pltpu.roll(weight_sides[side, q * HALF : (q + 1) * HALF], HALF, 1) for q in range(4)]
        head = weight_sides[side, 0:HALF] + kept(i > 0, turned[3])
        tail = turned[2] + kept(i < nr - 1, weight_sides[side, 4 * HALF : 5 * HALF])
        return jnp.concatenate([head, weight_sides[side, HALF : 3 * HALF], turned[0], turned[1], tail], axis=0)

    rights = (from_right, pltpu.roll(from_right, HALF, 1), weight_column(0))
    lefts = (from_left, pltpu.roll(from_left, HALF, 1), weight_column(1))
    for b in range(COLUMNS):
        sums = []
        for c in range(3):
            above = weight_rows[0, b] if c == 2 else rows_in[0, c, b]
            below = weight_rows[1, b] if c == 2 else rows_in[1, c, b]
            head = accum[c, b + 1, HALF:SIDE] + kept(i > 0, above)
            tail = accum[c, b + 1, TILE:low_edge] + kept(i < nr - 1, below)
            value = jnp.concatenate([head, accum[c, b + 1, SIDE:TILE], tail], axis=0)
            if b == 0:
                value = value + kept(jnp.logical_and(lane < HALF, j > 0), lefts[c])
            if b == COLUMNS - 1:
                value = value + kept(jnp.logical_and(lane >= HALF, j < nc - 1), rights[c])
            sums.append(value)
        part = slice(b * SIDE, (b + 1) * SIDE)
        for c in range(2):
            out[c, :, part] = obj[c, :, part] + sums[c] / (sums[2] + DAMPING)


def f32(*shape):
    return pltpu.VMEM(shape, jnp.float32)


def on_device(obj, probe, positions, counts, offsets, measured):
    nr, nc = lax.axis_size("row"), lax.axis_size("col")
    high, low = tables()
    dma = pltpu.SemaphoreType.DMA
    return pl.pallas_call(
        functools.partial(step_kernel, nr, nc),
        out_shape=pltpu.VMEM((2, TILE, TILE), jnp.float32),
        in_specs=[HBM] * 5 + [SMEM] * 3,
        out_specs=VMEM,
        scratch_shapes=[
            f32(2, TILE, TILE),
            f32(BEAMS, 2, SIDE, SIDE),
            f32(SCANS, SIDE, SIDE),
            pltpu.VMEM((2, 2 * SIDE, 2 * SIDE), jnp.bfloat16),
            pltpu.VMEM((2, 2 * SIDE, 2 * SIDE), jnp.bfloat16),
            pltpu.VMEM((SCANS, SIDE), jnp.int32),
            pltpu.VMEM((BEAMS, SCANS, SIDE), jnp.int32),
            pltpu.SMEM((BEAMS, SCANS, SIDE), jnp.int32),
            f32(2, SLABS, TALL, SIDE),
            f32(2, TALL, SIDE),
            f32(SCANS, BEAMS * SIDE, 2 * SIDE),
            f32(SCANS, 2 * SIDE, BEAMS * SIDE),
            f32(SCANS, BEAMS, SIDE, SIDE),
            f32(SCANS, 2, SIDE, SIDE),
            f32(SCANS, 2, SIDE, SIDE),
            f32(SCANS, BEAMS, SIDE, SIDE),
            f32(4 * BEAMS + 1, 2 * PAD, SIDE),
            f32(3, SLABS, TALL, SIDE),
            f32(2, 2, COLUMNS, HALF, SIDE),
            f32(2, TALL, SIDE),
            f32(2, 4 * HALF, SIDE),
            f32(2, COLUMNS, HALF, SIDE),
            f32(2, 5 * HALF, SIDE),
            dma((6,)),
            dma((31,)),
            dma((31,)),
            dma((SCANS, 8)),
            dma((SCANS, 7)),
        ],
        compiler_params=pltpu.CompilerParams(collective_id=1, has_side_effects=True, vmem_limit_bytes=54 * 2**20),
        name="step",
    )(obj, probe, measured[0, 0], jnp.asarray(high), jnp.asarray(low), positions[0, 0].T, counts, offsets.T)


def solution(mesh):
    return jax.shard_map(
        on_device,
        mesh=mesh,
        in_specs=(
            P(None, "row", "col"),
            P(),
            P("row", "col", None, None),
            P("row", "col"),
            P(),
            P("row", "col", None, None, None),
        ),
        out_specs=P(None, "row", "col"),
        check_vma=False,
    )
```

```python
import functools
import math

import jax
import jax.numpy as jnp
import numpy as np
from jax import lax
from jax.experimental import pallas as pl
from jax.experimental.pallas import tpu as pltpu
from jax.sharding import PartitionSpec as P

SIDE = 128
HALF = 64
BEAMS = 4
SCANS = 8
TILE = 384
TALL = TILE + 2 * HALF
COLUMNS = TILE // SIDE
SLABS = COLUMNS + 2
EPSILON = 0.5
DAMPING = 0.5
MESH = pl.DeviceIdType.MESH
VMEM = pl.BlockSpec(memory_space=pltpu.VMEM)
SMEM = pl.BlockSpec(memory_space=pltpu.SMEM)
HBM = pl.BlockSpec(memory_space=pltpu.HBM)
PAD = 512
STAGES = (("forward", 0), ("join", 1), ("settle", 2), ("hand_on", 3), ("back", 4))


def tables():
    index = np.arange(SIDE)
    angle = (index[:, None] * index[None, :] % SIDE) * (2.0 * math.pi / SIDE)
    c = np.cos(angle) / math.sqrt(SIDE)
    s = np.sin(angle) / math.sqrt(SIDE)
    lane = np.block([[c, -s], [s, c]])
    both = np.stack([lane, lane.T]).astype(np.float32)
    high = both.astype(jnp.bfloat16)
    low = (both - high.astype(np.float32)).astype(jnp.bfloat16)
    return high, low


def split(x):
    high = x.astype(jnp.bfloat16)
    return high, (x - high.astype(jnp.float32)).astype(jnp.bfloat16)


def dot(a, b):
    return jnp.dot(a, b, preferred_element_type=jnp.float32)


def on_lanes(x, high, low):
    x_high, x_low = split(x)
    return dot(x_high, high) + (dot(x_low, high) + dot(x_high, low))


def on_rows(high, low, x):
    x_high, x_low = split(x)
    return dot(high, x_high) + (dot(high, x_low) + dot(low, x_high))


def lane_start(x):
    at = x + HALF
    slab = lax.div(at, SIDE)
    return slab, at - slab * SIDE


def by_fourth(z, s):
    return jnp.where(z == 1, 0, jnp.where(z >= 2, 1, lax.rem(s, 2)))


def neighbours(i, j, nr, nc):
    up, down = lax.rem(i + nr - 1, nr), lax.rem(i + 1, nr)
    left, right = lax.rem(j + nc - 1, nc), lax.rem(j + 1, nc)
    return up, down, left, right


def step_kernel(
    nr, nc, obj_hbm, probe_hbm, measured_hbm, high_hbm, low_hbm, positions, counts, offsets, out,
    obj, probe, measured, high, low, meta, metas_in, metas, frame, pack, psi, far, inten, relay, gathered, facs,
    padded, accum, rows_in, sides_in, weight_pack, weight_rows, weight_sides, local, send, recv, wave_send, wave_recv,
):
    i, j = lax.axis_index("row"), lax.axis_index("col")
    up, down, left, right = neighbours(i, j, nr, nc)
    later = [lax.rem(i + k, nr) for k in (1, 2, 3)]
    earlier = [lax.rem(i + nr - k, nr) for k in (1, 2, 3)]
    corners = [{"row": r, "col": c} for r in (up, down) for c in (left, right)]
    partners = [{"row": r} for r in later + earlier] + [{"col": left}, {"col": right}] + corners
    barrier = pltpu.get_barrier_semaphore()
    for partner in partners:
        pl.semaphore_signal(barrier, inc=1, device_id=partner, device_id_type=MESH)
    fetches = [
        pltpu.make_async_copy(src, dst, local.at[q])
        for q, (src, dst) in enumerate(
            ((obj_hbm, obj), (probe_hbm, probe), (high_hbm, high), (low_hbm, low), (measured_hbm, measured))
        )
    ]
    for fetch in fetches:
        fetch.start()
    row, item = [lax.broadcasted_iota(jnp.int32, (SCANS, SIDE), d) for d in range(2)]
    packed = jnp.where(item == 2, counts[0, 0], 0)
    for s in range(SCANS):
        for c in range(2):
            packed = jnp.where(jnp.logical_and(row == s, item == c), positions[c, s], packed)
    meta[...] = packed
    metas_in[0] = packed
    fetches[0].wait()
    lane = lax.broadcasted_iota(jnp.int32, (TILE, SIDE), 1)
    low_edge, top, end, last = HALF + TILE, TILE - HALF, SLABS - 1, TILE - SIDE
    pack[0, HALF:low_edge] = jnp.where(lane < HALF, obj[0, :, 0:SIDE], pltpu.roll(obj[1, :, 0:SIDE], HALF, 1))
    pack[1, HALF:low_edge] = jnp.where(lane < HALF, pltpu.roll(obj[1, :, last:TILE], HALF, 1), obj[0, :, last:TILE])
    pl.semaphore_wait(barrier, len(partners))

    def exchange(plan, first):
        copies = [
            pltpu.make_async_remote_copy(
                src_ref=src,
                dst_ref=dst,
                send_sem=send.at[first + q],
                recv_sem=recv.at[first + q],
                device_id=dev,
                device_id_type=MESH,
            )
            for q, (src, dst, dev) in enumerate(plan)
        ]
        for one in copies:
            one.start()
        return copies

    heads, tails = slice(HALF, SIDE), slice(TILE, low_edge)
    plan = [(meta, metas_in.at[k + 1], {"row": later[k]}) for k in range(3)]
    for b in range(COLUMNS):
        part = slice(b * SIDE, (b + 1) * SIDE)
        plan.append((obj.at[:, 0:HALF, part], frame.at[:, b + 1, low_edge:TALL], {"row": up}))
        plan.append((obj.at[:, top:TILE, part], frame.at[:, b + 1, 0:HALF], {"row": down}))
    plan += [
        (pack.at[0, HALF:low_edge], frame.at[0, end, HALF:low_edge], {"col": left}),
        (pack.at[1, HALF:low_edge], frame.at[0, 0, HALF:low_edge], {"col": right}),
        (pack.at[0, heads], frame.at[0, end, low_edge:TALL], {"row": up, "col": left}),
        (pack.at[0, tails], frame.at[0, end, 0:HALF], {"row": down, "col": left}),
        (pack.at[1, heads], frame.at[0, 0, low_edge:TALL], {"row": up, "col": right}),
        (pack.at[1, tails], frame.at[0, 0, 0:HALF], {"row": down, "col": right}),
    ]
    copies = exchange(plan, 0)
    for b in range(COLUMNS):
        frame[:, b + 1, HALF:low_edge] = obj[:, :, b * SIDE : (b + 1) * SIDE]

    def clear(q, carry):
        padded[q] = jnp.zeros((2 * PAD, SIDE), jnp.float32)
        return carry

    lax.fori_loop(0, 4 * BEAMS + 1, clear, 0)

    def clear_sum(q, carry):
        accum[lax.div(q, SLABS), lax.rem(q, SLABS)] = jnp.zeros((TALL, SIDE), jnp.float32)
        return carry

    lax.fori_loop(0, 3 * SLABS, clear_sum, 0)
    for fetch in fetches[1:]:
        fetch.wait()
    for one in copies[:3]:
        one.wait()
    settled = pltpu.make_async_copy(metas_in, metas, local.at[5])
    settled.start()
    settled.wait()
    column = lax.broadcasted_iota(jnp.int32, (SIDE, SIDE), 1)

    def beam_at(s, k):
        beam = jnp.int32(0)
        for q in range(1, BEAMS):
            beam = jnp.where(offsets[q, s] == k, q, beam)
        return beam

    def place(s, channels):
        starts, picks = [], []
        for k in range(BEAMS):
            slab, shift = lane_start(metas[k, s, 1])
            starts.append(PAD - metas[k, s, 0])
            live = s < metas[k, 0, 2]
            for q, (channel, values) in enumerate(channels):
                turned = pltpu.roll(jnp.where(live, values[k], 0.0), shift, 1)
                at = 2 * (q * BEAMS + k)
                padded[at, PAD : PAD + SIDE] = jnp.where(column >= shift, turned, 0.0)
                padded[at + 1, PAD : PAD + SIDE] = jnp.where(column < shift, turned, 0.0)
            picks.append([jnp.where(slab == b, 0, jnp.where(slab + 1 == b, 1, 2)) for b in range(SLABS)])
        for q, (channel, values) in enumerate(channels):

            def add(row, carry, q=q, channel=channel):
                here = pl.ds(pl.multiple_of(row * HALF, HALF), HALF)
                for b in range(SLABS):
                    value = accum[channel, b, here]
                    for k in range(BEAMS):
                        at = jnp.where(picks[k][b] == 2, 4 * BEAMS, 2 * (q * BEAMS + k) + picks[k][b])
                        value = value + padded[at, pl.ds(starts[k] + row * HALF, HALF)]
                    accum[channel, b, here] = value
                return carry

            lax.fori_loop(0, TALL // HALF, add, 0)

    def weigh(s):
        values = []
        for k in range(BEAMS):
            beam = beam_at(s, k)
            p_re, p_im = probe[beam, 0], probe[beam, 1]
            values.append(p_re * p_re + p_im * p_im)
        place(s, [(2, values)])

    def weigh_one(s, carry):
        weigh(s)
        return carry

    lax.fori_loop(0, SCANS, weigh_one, 0)
    half_lane = lax.broadcasted_iota(jnp.int32, (HALF, SIDE), 1)
    folds = [(q * HALF, (q + 3) * HALF) for q in range(1, 4)] + [(0, low_edge)]
    for side, slab in ((0, 0), (1, end)):
        for q, (first, second) in enumerate(folds):
            straight = accum[2, slab, first : first + HALF]
            folded = pltpu.roll(accum[2, slab, second : second + HALF], HALF, 1)
            keep = half_lane >= HALF if side == 0 else half_lane < HALF
            weight_pack[side, q * HALF : (q + 1) * HALF] = jnp.where(keep, straight, folded)
    mid, fold_rows = slice(0, 3 * HALF), slice(3 * HALF, 4 * HALF)
    weight_plan = [
        (accum.at[2, 1:end, 0:HALF], weight_rows.at[1], {"row": up}),
        (accum.at[2, 1:end, low_edge:TALL], weight_rows.at[0], {"row": down}),
    ]
    for side, to_col in ((0, left), (1, right)):
        weight_plan += [
            (weight_pack.at[side, mid], weight_sides.at[side, mid], {"col": to_col}),
            (weight_pack.at[side, fold_rows], weight_sides.at[side, 4 * HALF : 5 * HALF], {"row": up, "col": to_col}),
            (weight_pack.at[side, fold_rows], weight_sides.at[side, fold_rows], {"row": down, "col": to_col}),
        ]
    weight_copies = exchange(weight_plan, 15)
    for one in copies[3:]:
        one.wait()
    for slab in (0, end):
        frame[1, slab] = pltpu.roll(frame[0, slab], HALF, 1)

    @pl.when(i == 0)
    def _():
        frame[:, :, 0:HALF] = jnp.zeros((2, SLABS, HALF, SIDE), jnp.float32)

    @pl.when(i == nr - 1)
    def _():
        frame[:, :, low_edge:TALL] = jnp.zeros((2, SLABS, HALF, SIDE), jnp.float32)

    @pl.when(j == 0)
    def _():
        frame[:, 0] = jnp.zeros((2, TALL, SIDE), jnp.float32)

    @pl.when(j == nc - 1)
    def _():
        frame[:, end] = jnp.zeros((2, TALL, SIDE), jnp.float32)

    def to(by):
        return {"row": lax.rem(i + by + nr, nr)}

    def by_third(s, k):
        return by_fourth(lax.rem(i + nr - k, 4), s)

    def copy(s, kind):
        if kind == 0:
            src, dst, dev = inten.at[s, 2], relay.at[s, 0], to(-1)
        elif kind == 1:
            src, dst, dev = inten.at[s, 2], relay.at[s, 1], to(1)
        elif kind == 2:
            src, dst, dev = inten.at[s, 1], gathered.at[s, 0], to(-1)
        elif kind == 3:
            src, dst, dev = inten.at[s, 3], gathered.at[s, 1], to(-3)
        elif kind == 4:
            src, dst, dev = facs.at[s, 0], facs.at[s, 1], to(1)
        elif kind == 5:
            src, dst, dev = facs.at[s, 0], facs.at[s, 3], to(3)
        elif kind == 6:
            src, dst, dev = facs.at[s, 1], facs.at[s, 2], to(1)
        else:
            src, dst, dev = facs.at[s, 3], facs.at[s, 2], to(-1)
        place = 6 if kind == 7 else kind
        return pltpu.make_async_remote_copy(
            src_ref=src,
            dst_ref=dst,
            send_sem=wave_send.at[s, kind],
            recv_sem=wave_recv.at[s, place],
            device_id=dev,
            device_id_type=MESH,
        )

    def forward(s):
        rows = []
        for k in range(BEAMS):
            y = metas[k, s, 0]
            slab, shift = lane_start(metas[k, s, 1])
            turn = lax.rem(SIDE - shift, SIDE)
            beam = beam_at(s, k)
            z_re, z_im = [
                jnp.where(
                    column < SIDE - shift,
                    pltpu.roll(frame[c, slab, pl.ds(y, SIDE)], turn, 1),
                    pltpu.roll(frame[c, slab + 1, pl.ds(y, SIDE)], turn, 1),
                )
                for c in range(2)
            ]
            p_re, p_im = probe[beam, 0], probe[beam, 1]
            wave = jnp.concatenate([p_re * z_re - p_im * z_im, p_re * z_im + p_im * z_re], axis=1)
            psi[s, k * SIDE : (k + 1) * SIDE] = wave
            rows.append(wave)
        once = on_lanes(jnp.concatenate(rows, axis=0), high[0], low[0])
        once = jnp.concatenate(
            [
                jnp.concatenate([once[k * SIDE : (k + 1) * SIDE, q * SIDE : (q + 1) * SIDE] for k in range(BEAMS)], axis=1)
                for q in range(2)
            ],
            axis=0,
        )
        twice = on_rows(high[1], low[1], once)
        far[s] = twice
        for k in (2, 1, 3, 0):
            re = twice[:SIDE, k * SIDE : (k + 1) * SIDE]
            im = twice[SIDE:, k * SIDE : (k + 1) * SIDE]
            inten[s, k] = re * re + im * im
        for kind, wanted in ((0, by_third(s, 2) == 0), (1, by_third(s, 2) == 1), (2, by_third(s, 1) == 1), (3, by_third(s, 3) == 0)):

            @pl.when(wanted)
            def _(kind=kind):
                copy(s, kind).start()

    def join(s):
        for k, which, wanted in ((1, 0, by_third(s, 1) == 0), (3, 1, by_third(s, 3) == 1)):

            @pl.when(wanted)
            def _(k=k, which=which):
                copy(s, which).wait_recv()
                inten[s, k] = inten[s, k] + relay[s, which]
                copy(s, 2 + which).start()

    def settle(s):
        copy(s, 2).wait_recv()
        copy(s, 3).wait_recv()
        total = inten[s, 0] + gathered[s, 0] + gathered[s, 1]
        facs[s, 0] = measured[s] / jnp.sqrt(total + EPSILON)
        copy(s, 4).start()
        copy(s, 5).start()

    def hand_on(s):
        for k, which, wanted in ((1, 0, by_third(s, 1) == 0), (3, 1, by_third(s, 3) == 1)):

            @pl.when(wanted)
            def _(k=k, which=which):
                copy(s, 4 + which).wait_recv()
                copy(s, 6 + which).start()

    def back(s):
        for k, which, wanted in ((1, 0, by_third(s, 1) == 1), (3, 1, by_third(s, 3) == 0)):

            @pl.when(wanted)
            def _(which=which):
                copy(s, 4 + which).wait_recv()

        copy(s, 6).wait_recv()
        factor = jnp.concatenate([facs[s, k] for k in range(BEAMS)], axis=1)
        scaled = jnp.concatenate([far[s, :SIDE] * factor, far[s, SIDE:] * factor], axis=0)
        once = on_rows(high[0], low[0], scaled)
        once = jnp.concatenate(
            [
                jnp.concatenate([once[q * SIDE : (q + 1) * SIDE, k * SIDE : (k + 1) * SIDE] for q in range(2)], axis=1)
                for k in range(BEAMS)
            ],
            axis=0,
        )
        change = on_lanes(once, high[1], low[1]) - psi[s]
        re, im = [], []
        for k in range(BEAMS):
            beam = beam_at(s, k)
            p_re, p_im = probe[beam, 0], probe[beam, 1]
            c_re = change[k * SIDE : (k + 1) * SIDE, :SIDE]
            c_im = change[k * SIDE : (k + 1) * SIDE, SIDE:]
            re.append(p_re * c_re + p_im * c_im)
            im.append(p_re * c_im - p_im * c_re)
        place(s, [(0, re), (1, im)])

    ends = ((0, HALF, low_edge, up), (HALF, low_edge, HALF, None), (low_edge, TALL, 0, down))
    sides = ((0, left), (end, right))
    rim_plan = [
        (accum.at[0:2, 1:end, 0:HALF], rows_in.at[1], {"row": up}),
        (accum.at[0:2, 1:end, low_edge:TALL], rows_in.at[0], {"row": down}),
    ]
    for side, (slab, to_col) in enumerate(sides):
        for first, stop, land, to_row in ends:
            dev = {"col": to_col} if to_row is None else {"row": to_row, "col": to_col}
            arrive = slice(land, land + stop - first)
            rim_plan.append((pack.at[side, first:stop], sides_in.at[side, arrive], dev))
    work = {"forward": forward, "join": join, "settle": settle, "hand_on": hand_on, "back": back}

    def step(t, carry):
        for name, lag in STAGES:

            @pl.when(jnp.logical_and(t >= lag, t < SCANS + lag))
            def _(name=name, lag=lag):
                work[name](t - lag)

        return carry

    lax.fori_loop(0, SCANS + STAGES[-1][1], step, 0)
    lane = lax.broadcasted_iota(jnp.int32, (TALL, SIDE), 1)
    pack[0] = jnp.where(lane >= HALF, accum[0, 0], pltpu.roll(accum[1, 0], HALF, 1))
    pack[1] = jnp.where(lane < HALF, accum[0, end], pltpu.roll(accum[1, end], HALF, 1))
    copies = exchange(rim_plan, 23)
    for one in weight_copies:
        one.wait()

    def drain(s, carry):
        for kind in (2, 3, 4, 5):
            copy(s, kind).wait_send()
        for kind, wanted in (
            (0, by_third(s, 2) == 0),
            (1, by_third(s, 2) == 1),
            (6, by_third(s, 1) == 0),
            (7, by_third(s, 3) == 1),
        ):

            @pl.when(wanted)
            def _(kind=kind):
                copy(s, kind).wait_send()

        return carry

    lax.fori_loop(0, SCANS, drain, 0)
    for one in copies:
        one.wait()

    def kept(ok, value):
        return jnp.where(ok, value, 0.0)

    lane = lax.broadcasted_iota(jnp.int32, (TILE, SIDE), 1)

    def rim_column(ref, side):
        head = ref[side, HALF:SIDE] + kept(i > 0, ref[side, 0:HALF])
        tail = ref[side, TILE:low_edge] + kept(i < nr - 1, ref[side, low_edge:TALL])
        return jnp.concatenate([head, ref[side, SIDE:TILE], tail], axis=0)

    from_right, from_left = rim_column(sides_in, 0), rim_column(sides_in, 1)

    def weight_column(side):
        turned = [pltpu.roll(weight_sides[side, q * HALF : (q + 1) * HALF], HALF, 1) for q in range(4)]
        head = weight_sides[side, 0:HALF] + kept(i > 0, turned[3])
        tail = turned[2] + kept(i < nr - 1, weight_sides[side, 4 * HALF : 5 * HALF])
        return jnp.concatenate([head, weight_sides[side, HALF : 3 * HALF], turned[0], turned[1], tail], axis=0)

    rights = (from_right, pltpu.roll(from_right, HALF, 1), weight_column(0))
    lefts = (from_left, pltpu.roll(from_left, HALF, 1), weight_column(1))
    for b in range(COLUMNS):
        sums = []
        for c in range(3):
            above = weight_rows[0, b] if c == 2 else rows_in[0, c, b]
            below = weight_rows[1, b] if c == 2 else rows_in[1, c, b]
            head = accum[c, b + 1, HALF:SIDE] + kept(i > 0, above)
            tail = accum[c, b + 1, TILE:low_edge] + kept(i < nr - 1, below)
            value = jnp.concatenate([head, accum[c, b + 1, SIDE:TILE], tail], axis=0)
            if b == 0:
                value = value + kept(jnp.logical_and(lane < HALF, j > 0), lefts[c])
            if b == COLUMNS - 1:
                value = value + kept(jnp.logical_and(lane >= HALF, j < nc - 1), rights[c])
            sums.append(value)
        part = slice(b * SIDE, (b + 1) * SIDE)
        for c in range(2):
            out[c, :, part] = obj[c, :, part] + sums[c] / (sums[2] + DAMPING)


def f32(*shape):
    return pltpu.VMEM(shape, jnp.float32)


def on_device(obj, probe, positions, counts, offsets, measured):
    nr, nc = lax.axis_size("row"), lax.axis_size("col")
    high, low = tables()
    dma = pltpu.SemaphoreType.DMA
    return pl.pallas_call(
        functools.partial(step_kernel, nr, nc),
        out_shape=pltpu.VMEM((2, TILE, TILE), jnp.float32),
        in_specs=[HBM] * 5 + [SMEM] * 3,
        out_specs=VMEM,
        scratch_shapes=[
            f32(2, TILE, TILE),
            f32(BEAMS, 2, SIDE, SIDE),
            f32(SCANS, SIDE, SIDE),
            pltpu.VMEM((2, 2 * SIDE, 2 * SIDE), jnp.bfloat16),
            pltpu.VMEM((2, 2 * SIDE, 2 * SIDE), jnp.bfloat16),
            pltpu.VMEM((SCANS, SIDE), jnp.int32),
            pltpu.VMEM((BEAMS, SCANS, SIDE), jnp.int32),
            pltpu.SMEM((BEAMS, SCANS, SIDE), jnp.int32),
            f32(2, SLABS, TALL, SIDE),
            f32(2, TALL, SIDE),
            f32(SCANS, BEAMS * SIDE, 2 * SIDE),
            f32(SCANS, 2 * SIDE, BEAMS * SIDE),
            f32(SCANS, BEAMS, SIDE, SIDE),
            f32(SCANS, 2, SIDE, SIDE),
            f32(SCANS, 2, SIDE, SIDE),
            f32(SCANS, BEAMS, SIDE, SIDE),
            f32(4 * BEAMS + 1, 2 * PAD, SIDE),
            f32(3, SLABS, TALL, SIDE),
            f32(2, 2, COLUMNS, HALF, SIDE),
            f32(2, TALL, SIDE),
            f32(2, 4 * HALF, SIDE),
            f32(2, COLUMNS, HALF, SIDE),
            f32(2, 5 * HALF, SIDE),
            dma((6,)),
            dma((31,)),
            dma((31,)),
            dma((SCANS, 8)),
            dma((SCANS, 7)),
        ],
        compiler_params=pltpu.CompilerParams(collective_id=1, has_side_effects=True, vmem_limit_bytes=54 * 2**20),
        name="step",
    )(obj, probe, measured[0, 0], jnp.asarray(high), jnp.asarray(low), positions[0, 0].T, counts, offsets.T)


def solution(mesh):
    return jax.shard_map(
        on_device,
        mesh=mesh,
        in_specs=(
            P(None, "row", "col"),
            P(),
            P("row", "col", None, None),
            P("row", "col"),
            P(),
            P("row", "col", None, None, None),
        ),
        out_specs=P(None, "row", "col"),
        check_vma=False,
    )
```
